512 devices in a mesh: dp: 8 (over z), fsdp: 64 (over y, x, core).
Axes of the slice: x: 4, y: 8, z: 8, core: 2. Of those that a mesh axis runs over, the one named last changes fastest.
Arguments:
- small_cols: bfloat16 [393216, 128], P(('dp', 'fsdp')), may hold values from -24 to 24
- wide_cols: bfloat16 [393216, 2, 1536], P(('dp', 'fsdp')), may hold values from -24 to 24
- token_counts: int32 [512], P(('dp', 'fsdp')), may hold values from 144 to 768, as said below
- loss_sums: float32 [512], P(('dp', 'fsdp'))
- weight: float32 [128, 1536], P('fsdp'), may hold values from -0.75 to 0.75
- first_moment: float32 [128, 1536], P('fsdp'), may hold values from -0.002 to 0.002
- second_moment: float32 [128, 1536], P('fsdp'), may hold values from 1e-07 to 1e-06
- step: int32 [], replicated, may hold values from 1 to 2999
Outputs:
- new_weight: float32 [128, 1536], P('fsdp')
- new_first: float32 [128, 1536], P('fsdp')
- new_second: float32 [128, 1536], P('fsdp')
- adam_step: float32 [128, 1536], P('fsdp')
- grad_norm: float32 [], replicated
- mean_loss: float32 [], replicated
The draws below stay inside these ranges and needn't reach their ends.
Inputs may be any that keep to these rules, and one draw needn't show every extreme that they name: `token_counts`: each count is f * h * w with f from 1 to 3 and h, w from 12 to 16; in every draw some device's count is exactly 768.
All inputs are finite; a program needn't handle non-finite values.
Results may differ from the reference program's by a relative error of at most 0.0003.
Values sent between devices are 32-bit elements; how exact they have to be, the bound alone decides.
No kernel may reach another device: no remote copies, remote signals or barrier semaphores. Data moves between devices by JAX's collectives and lax.ppermute only.
A program may use at most 64 MiB of HBM per device.

```python
import math
import jax
import jax.numpy as jnp
from jax import lax

D = 1536
PATCH = 64
FRAMES = 3
GRID = 16
CAP = 768
ROWS = 128
DEVS = 512


def draw_token_counts(key, part):
    keys = jax.random.split(jax.random.fold_in(key, 11), 4)
    frames = jax.random.randint(keys[0], (DEVS,), 1, FRAMES + 1)
    heights = jax.random.randint(keys[1], (DEVS,), 3 * GRID // 4, GRID + 1)
    widths = jax.random.randint(keys[2], (DEVS,), 3 * GRID // 4, GRID + 1)
    chosen = jax.random.randint(keys[3], (), 0, DEVS)
    counts = frames * heights * widths
    fullest = jnp.full((DEVS,), FRAMES * GRID * GRID, jnp.int32)
    return jnp.where(jnp.arange(DEVS) == chosen, fullest, counts).astype(jnp.int32)


def draw_loss_sums(key, part):
    keys = jax.random.split(jax.random.fold_in(key, 23), 1)
    ramp = 1.0 + 2.0 * jnp.arange(DEVS, dtype=jnp.float32) / max(DEVS - 1, 1)
    spread = jax.random.uniform(keys[0], (DEVS,), jnp.float32, 0.5, 1.5)
    values = 300.0 * ramp * spread
    return jnp.maximum(values, 10.0).astype(jnp.float32)


def with_spikes(drawn, own_key, source, target, parts, factor):
    def block_of(position):
        return (jnp.arange(drawn.shape[position]) // (drawn.shape[position] // parts)).reshape((-1,) + (1,) * (drawn.ndim - 1 - position))

    near = jax.random.permutation(own_key, parts)[block_of(target)]
    other_side = (block_of(target) + parts // 2) % parts
    return jnp.where((block_of(source) == near) | (block_of(source) == other_side), factor * drawn, drawn)


def steps_of(stream_key, shape, cuts, low, top_value):
    factor_of, own = 1.0, jax.random.fold_in(stream_key, 6)
    for axis_at, parts in cuts:
        steps = jnp.exp(jax.random.uniform(jax.random.fold_in(own, axis_at), (parts,), jnp.float32, low / len(cuts), top_value / len(cuts)))
        factor_of = factor_of * jnp.repeat(steps, shape[axis_at] // parts).reshape([-1 if axis == axis_at else 1 for axis in range(len(shape))])
    return factor_of


def gaussian(rng, dims, width, bound, cuts=(), held_as=jnp.bfloat16):
    drawn = width * jax.random.normal(rng, dims, jnp.float32)
    if cuts:
        drawn = drawn * steps_of(rng, dims, cuts, -0.22, 0.18)
    return jnp.clip(drawn, -bound, bound).astype(held_as)


def bell_draw_with(stream_key, extent, deviation, limit, cuts, heavy, kind=jnp.bfloat16):
    result = deviation * jax.random.normal(stream_key, extent, jnp.float32)
    if cuts:
        result = result * steps_of(stream_key, extent, cuts, -0.22, 0.18)
    return jnp.clip(with_spikes(result, jax.random.fold_in(stream_key, 3), *heavy), -limit, limit).astype(kind)


def setup_inputs(seed: int = 0) -> dict:
    splits = jax.random.split(jax.random.key(seed), 9)
    return {
        "small_cols": bell_draw_with(splits[0], (DEVS * CAP, ROWS), 1.0, 24.0, ((0, 512),), (0, 1, 128, 5.5)),
        "wide_cols": gaussian(splits[1], (DEVS * CAP, 2, D), 4.0, 24.0, ((0, 512),)),
        "token_counts": draw_token_counts(jax.random.fold_in(splits[8], 71), 0),
        "loss_sums": draw_loss_sums(jax.random.fold_in(splits[8], 71), 0),
        "weight": gaussian(splits[4], (ROWS, D), PATCH ** -0.5, 0.75, ((0, 64),), jnp.float32),
        "first_moment": gaussian(splits[5], (ROWS, D), 0.0003, 0.002, ((0, 64),), jnp.float32),
        "second_moment": jnp.clip(jnp.exp(math.log(9.999999974752427e-07) - 2.3025851 * jax.random.uniform(splits[6], (ROWS, D), jnp.float32) ** steps_of(splits[6], (ROWS, D), ((0, 64),), -0.2, 0.2)), 1.0000000116860974e-07, 9.999999974752427e-07),
        "step": jax.random.randint(splits[7], (), 1, 3000).astype(jnp.int32),
    }


MAX_NORM = 1.0
BETA_FIRST = 0.9
BETA_SECOND = 0.999
EPSILON_ADAM = 1e-08
LEARN_RATE = 0.02
DECAY_RATE = 0.1

def reference(small_cols, wide_cols, token_counts, loss_sums, weight, first_moment, second_moment, step):
    positions = jnp.arange(CAP, dtype=jnp.int32)

    def add_device(running, device):
        offset = (device * CAP).astype(jnp.int32)
        narrow = lax.dynamic_slice_in_dim(small_cols, offset, CAP, 0).astype(jnp.float32)
        broad = lax.dynamic_slice_in_dim(wide_cols, offset, CAP, 0).astype(jnp.float32)
        is_live = positions < token_counts[device]
        narrow = jnp.where(is_live[:, None], narrow, jnp.zeros_like(narrow))
        portion = jnp.einsum('thc,thd->hcd', narrow.reshape(CAP, 2, PATCH), broad)
        return (running + portion.reshape(ROWS, D), None)
    raw_sum, unused = lax.scan(add_device, jnp.zeros((ROWS, D), jnp.float32), jnp.arange(DEVS, dtype=jnp.int32))
    token_total = jnp.sum(token_counts.astype(jnp.float32))
    loss_total = jnp.sum(loss_sums)
    gradient = raw_sum / token_total
    grad_norm = jnp.sqrt(jnp.sum(gradient * gradient))
    mean_loss = loss_total / token_total
    clip_factor = jnp.minimum(1.0, MAX_NORM / (grad_norm + 1e-06))
    clipped = gradient * clip_factor
    new_first = BETA_FIRST * first_moment + (1.0 - BETA_FIRST) * clipped
    new_second = BETA_SECOND * second_moment + (1.0 - BETA_SECOND) * clipped * clipped
    step_float = step.astype(jnp.float32)
    first_hat = new_first / (1.0 - jnp.power(jnp.float32(BETA_FIRST), step_float))
    second_hat = new_second / (1.0 - jnp.power(jnp.float32(BETA_SECOND), step_float))
    adam_step = first_hat / (jnp.sqrt(second_hat) + EPSILON_ADAM) + DECAY_RATE * weight
    new_weight = weight - LEARN_RATE * adam_step
    return (new_weight, new_first, new_second, adam_step, grad_norm, mean_loss)
```

```python
import functools
import math

import jax
import jax.numpy as jnp
from jax import lax
from jax.experimental import pallas as pl
from jax.experimental.pallas import tpu as pltpu
from jax.sharding import PartitionSpec as P

MAX_NORM = 1.0
BETA_FIRST = 0.9
BETA_SECOND = 0.999
EPSILON_ADAM = 1e-08
LEARN_RATE = 0.02
DECAY_RATE = 0.1
LOG_FIRST = -0.10536054214877988
LOG_SECOND = -0.0010004874460928543

LANES = 128
STEP_TOKENS = 128
VMEM = pl.BlockSpec(memory_space=pltpu.VMEM)
HBM = pl.BlockSpec(memory_space=pltpu.HBM)
ANY = pl.BlockSpec(memory_space=pl.ANY)


def in_hbm(array):
    return pltpu.with_memory_space_constraint(array, pltpu.HBM)


def correction(step, log_beta):
    u = step * log_beta
    series = jnp.ones_like(u)
    for k in range(11, 1, -1):
        series = 1.0 + (u / k) * series
    return jnp.where(u > -0.5, -u * series, 1.0 - jnp.exp(u))


def term_kernel(
    count_ref,
    loss_ref,
    step_ref,
    small_ref,
    wide_ref,
    keep_ref,
    send_ref,
    extra_ref,
    small_vmem,
    wide_vmem,
    total,
    count_held,
    loss_held,
    step_held,
    sems,
    small_sems,
):
    tokens, width = small_ref.shape
    steps = sems.shape[0]
    each = tokens // steps
    core = lax.rem(lax.axis_index("fsdp"), 2)
    first = [
        pltpu.make_async_copy(ref, held, small_sems.at[i])
        for i, (ref, held) in enumerate(
            (
                (count_ref, count_held),
                (small_ref, small_vmem),
                (loss_ref, loss_held),
                (step_ref, step_held),
            )
        )
    ]
    copies = [
        pltpu.make_async_copy(
            wide_ref.at[pl.ds(i * each, each)], wide_vmem.at[pl.ds(i * each, each)], sems.at[i]
        )
        for i in range(steps)
    ]
    for c in first[:2] + copies + first[2:]:
        c.start()
    first[0].wait()
    live = count_held[...]
    first[1].wait()
    tiles = total.shape[0]
    for i in range(steps):
        copies[i].wait()
        row = lax.broadcasted_iota(jnp.int32, (2 * each, each), 0)
        col = lax.broadcasted_iota(jnp.int32, (2 * each, each), 1)
        twice = jnp.where((row // 2 == col) & (col + i * each < live), 1.0, 0.0).astype(jnp.bfloat16)
        narrow = jnp.dot(
            twice, small_vmem[i * each : (i + 1) * each, :], preferred_element_type=jnp.float32
        )
        row = lax.broadcasted_iota(jnp.int32, (2 * each, width), 0)
        col = lax.broadcasted_iota(jnp.int32, (2 * each, width), 1)
        narrow = jnp.where(row % 2 == col // (width // 2), narrow, 0.0).astype(jnp.bfloat16)
        broad = wide_vmem[i * each : (i + 1) * each].reshape(2 * each, tiles * LANES)
        term = lax.dot_general(
            narrow, broad, (((0,), (0,)), ((), ())), preferred_element_type=jnp.float32
        )
        for t in range(tiles):
            part = term[:, t * LANES : (t + 1) * LANES]
            total[t] = part if i == 0 else total[t] + part
    first[2].wait()
    first[3].wait()
    lane = lax.broadcasted_iota(jnp.int32, (1, LANES), 1)
    step = step_held[...].astype(jnp.float32)
    scales = correction(step, jnp.where(lane == 3, LOG_FIRST, LOG_SECOND))
    extra = jnp.where(lane == 0, live.astype(jnp.float32), jnp.where(lane == 1, loss_held[...], scales))
    extra_ref[...] = jnp.broadcast_to(extra, extra_ref.shape)
    owners = keep_ref.shape[0]
    for t in range(tiles):
        for j in range(2):
            even = total[t, pl.ds(j, owners, stride=4), :]
            odd = total[t, pl.ds(2 + j, owners, stride=4), :]
            keep_ref[:, 2 * t + j, :] = jnp.where(core == 0, even, odd)
            send_ref[:, 2 * t + j, :] = jnp.where(core == 0, odd, even)


def device_term(small_cols, wide_cols, token_counts, loss_sums, step):
    tokens, width = small_cols.shape
    d = wide_cols.shape[2]
    half = jax.ShapeDtypeStruct((width // 4, 2 * d // LANES, LANES), jnp.float32)
    return pl.pallas_call(
        term_kernel,
        out_shape=(half, half, jax.ShapeDtypeStruct((8, LANES), jnp.float32)),
        in_specs=[ANY] * 3 + [HBM] * 2,
        out_specs=(VMEM, VMEM, VMEM),
        scratch_shapes=[
            pltpu.VMEM((tokens, width), jnp.bfloat16),
            pltpu.VMEM((tokens, 2, d), jnp.bfloat16),
            pltpu.VMEM((d // LANES, width, LANES), jnp.float32),
            pltpu.VMEM((1, 1), jnp.int32),
            pltpu.VMEM((1, 1), jnp.float32),
            pltpu.VMEM((1, 1), jnp.int32),
            pltpu.SemaphoreType.DMA((tokens // STEP_TOKENS,)),
            pltpu.SemaphoreType.DMA((4,)),
        ],
        compiler_params=pltpu.CompilerParams(vmem_limit_bytes=16 * 2**20),
        name="term",
    )(*(a.reshape(1, 1) for a in (token_counts, loss_sums, step)), in_hbm(small_cols), in_hbm(wide_cols))


def owned_kernel(extra_ref, parts_ref, out_ref):
    rows = parts_ref.shape[1]
    total = jnp.sum(parts_ref[...], axis=0)
    extra = extra_ref[...]
    for k in range(out_ref.shape[0]):
        out_ref[k, 0:rows, :] = total
        out_ref[k, rows:, :] = extra


def owned(extra, parts, replicas):
    rows = parts.shape[1] + extra.shape[0]
    return pl.pallas_call(
        owned_kernel,
        out_shape=jax.ShapeDtypeStruct((replicas, rows, LANES), jnp.float32),
        in_specs=[VMEM, VMEM],
        out_specs=VMEM,
        compiler_params=pltpu.CompilerParams(vmem_limit_bytes=4 * 2**20),
        name="owned",
    )(extra, parts)


def square_kernel(parts_ref, summed_ref, message_ref):
    rows = summed_ref.shape[0]
    total = jnp.sum(parts_ref[...], axis=0)
    summed = total[:rows]
    summed_ref[...] = summed
    squares = jnp.sum(summed * summed)
    lane = lax.broadcasted_iota(jnp.int32, (1, LANES), 1)
    shifted = total[rows : rows + 1]
    message = jnp.where(lane == 2, squares, shifted)
    message_ref[...] = jnp.broadcast_to(message, message_ref.shape)


def square(parts, owners):
    rows = parts.shape[1] - 8
    return pl.pallas_call(
        square_kernel,
        out_shape=(
            jax.ShapeDtypeStruct((rows, LANES), jnp.float32),
            jax.ShapeDtypeStruct((owners, LANES), jnp.float32),
        ),
        in_specs=[VMEM],
        out_specs=(VMEM, VMEM),
        compiler_params=pltpu.CompilerParams(vmem_limit_bytes=4 * 2**20),
        name="square",
    )(parts)


def update_kernel(
    extra_ref,
    message_ref,
    summed_ref,
    weight_ref,
    first_ref,
    second_ref,
    new_weight_ref,
    new_first_ref,
    new_second_ref,
    adam_ref,
    norm_ref,
    loss_ref,
    rows_ref,
):
    first_scale, second_scale = extra_ref[0:1, 3:4], extra_ref[0:1, 4:5]
    sums = jnp.sum(message_ref[...], axis=0, keepdims=True)
    lane = lax.broadcasted_iota(jnp.int32, sums.shape, 1)

    def take(k):
        return jnp.sum(jnp.where(lane == k, sums, 0.0), axis=1, keepdims=True)

    token_total, loss_total, squares = take(0), take(1), take(2)
    grad_norm = jnp.sqrt(squares) / token_total
    clip = jnp.minimum(1.0, MAX_NORM / (grad_norm + 1e-06))
    norm_ref[...] = grad_norm
    loss_ref[...] = loss_total / token_total
    for t in range(rows_ref.shape[1] // LANES):
        rows_ref[:, t * LANES : (t + 1) * LANES] = summed_ref[2 * t : 2 * t + 2, :]
    clipped = rows_ref[...] / token_total * clip
    new_first = BETA_FIRST * first_ref[...] + (1.0 - BETA_FIRST) * clipped
    new_second = BETA_SECOND * second_ref[...] + (1.0 - BETA_SECOND) * clipped * clipped
    first_hat = new_first / first_scale
    second_hat = new_second / second_scale
    weight = weight_ref[...]
    adam = first_hat / (jnp.sqrt(second_hat) + EPSILON_ADAM) + DECAY_RATE * weight
    new_weight_ref[...] = weight - LEARN_RATE * adam
    new_first_ref[...] = new_first
    new_second_ref[...] = new_second
    adam_ref[...] = adam


def update(extra, message, summed, weight, first_moment, second_moment):
    state = jax.ShapeDtypeStruct(weight.shape, jnp.float32)
    scalar = jax.ShapeDtypeStruct((1, 1), jnp.float32)
    return pl.pallas_call(
        update_kernel,
        out_shape=(state, state, state, state, scalar, scalar),
        in_specs=[VMEM] * 6,
        out_specs=(VMEM,) * 6,
        scratch_shapes=[pltpu.VMEM(weight.shape, jnp.float32)],
        compiler_params=pltpu.CompilerParams(vmem_limit_bytes=4 * 2**20),
        name="update",
    )(extra, message, summed, weight, first_moment, second_moment)


def on_device(
    small_cols, wide_cols, token_counts, loss_sums, weight, first_moment, second_moment, step
):
    owners, replicas = lax.axis_size("fsdp"), lax.axis_size("dp")
    keep, send, extra = device_term(small_cols, wide_cols, token_counts, loss_sums, step)
    partner = [(i, i ^ 1) for i in range(owners)]
    chip_sum = keep + lax.ppermute(send, "fsdp", partner)
    same_core = [list(range(c, owners, 2)) for c in range(2)]
    parts = lax.all_to_all(chip_sum, "fsdp", 0, 0, axis_index_groups=same_core, tiled=True)
    parts = lax.all_to_all(owned(extra, parts, replicas), "dp", 0, 0, tiled=True)
    summed, message = square(parts, owners)
    message = lax.all_to_all(message[:, None, :], "fsdp", 0, 0, tiled=True)[:, 0, :]
    new_weight, new_first, new_second, adam_step, grad_norm, mean_loss = update(
        extra,
        message,
        summed,
        weight,
        first_moment,
        second_moment,
    )
    return (
        new_weight,
        new_first,
        new_second,
        adam_step,
        grad_norm.reshape(()),
        mean_loss.reshape(()),
    )


def solution(mesh):
    in_specs = (
        P(("dp", "fsdp"), None),
        P(("dp", "fsdp"), None, None),
        P(("dp", "fsdp")),
        P(("dp", "fsdp")),
        P("fsdp", None),
        P("fsdp", None),
        P("fsdp", None),
        P(),
    )
    out_specs = (P("fsdp", None), P("fsdp", None), P("fsdp", None), P("fsdp", None), P(), P())
    return jax.shard_map(
        on_device, mesh=mesh, in_specs=in_specs, out_specs=out_specs, check_vma=False
    )
```

```python
import functools
import math

import jax
import jax.numpy as jnp
from jax import lax
from jax.experimental import pallas as pl
from jax.experimental.pallas import tpu as pltpu
from jax.sharding import PartitionSpec as P

MAX_NORM = 1.0
BETA_FIRST = 0.9
BETA_SECOND = 0.999
EPSILON_ADAM = 1e-08
LEARN_RATE = 0.02
DECAY_RATE = 0.1
LOG_FIRST = -0.10536054214877988
LOG_SECOND = -0.0010004874460928543

LANES = 128
STEP_TOKENS = 384
VMEM = pl.BlockSpec(memory_space=pltpu.VMEM)
HBM = pl.BlockSpec(memory_space=pltpu.HBM)
SMEM = pl.BlockSpec(memory_space=pltpu.SMEM)


def in_hbm(array):
    return pltpu.with_memory_space_constraint(array, pltpu.HBM)


def term_kernel(
    count_ref,
    small_ref,
    wide_ref,
    keep_ref,
    send_ref,
    small_vmem,
    wide_vmem,
    narrow,
    total,
    sems,
    small_sem,
):
    tokens, width = small_ref.shape
    steps = sems.shape[0]
    each = tokens // steps
    core = lax.rem(lax.axis_index("fsdp"), 2)
    small_copy = pltpu.make_async_copy(small_ref, small_vmem, small_sem)
    copies = [
        pltpu.make_async_copy(
            wide_ref.at[pl.ds(i * each, each)], wide_vmem.at[pl.ds(i * each, each)], sems.at[i]
        )
        for i in range(steps)
    ]
    small_copy.start()
    for c in copies:
        c.start()
    live = count_ref[0]
    small_copy.wait()
    block = 128
    for i in range(tokens // block):
        token = lax.broadcasted_iota(jnp.int32, (block, 2 * block), 0)
        slot = lax.broadcasted_iota(jnp.int32, (block, 2 * block), 1)
        twice = jnp.where((slot // 2 == token) & (token + i * block < live), 1.0, 0.0)
        rows = lax.dot_general(
            small_vmem[i * block : (i + 1) * block, :],
            twice.astype(jnp.bfloat16),
            (((0,), (0,)), ((), ())),
            preferred_element_type=jnp.float32,
        )
        row = lax.broadcasted_iota(jnp.int32, (width, 2 * block), 0)
        slot = lax.broadcasted_iota(jnp.int32, (width, 2 * block), 1)
        rows = jnp.where(slot % 2 == row // (width // 2), rows, 0.0)
        narrow[:, 2 * block * i : 2 * block * (i + 1)] = rows.astype(jnp.bfloat16)
    tiles = total.shape[0]
    for i in range(steps):
        copies[i].wait()
        broad = wide_vmem[i * each : (i + 1) * each].reshape(2 * each, tiles * LANES)
        term = jnp.dot(
            narrow[:, 2 * each * i : 2 * each * (i + 1)], broad, preferred_element_type=jnp.float32
        )
        for t in range(tiles):
            part = term[:, t * LANES : (t + 1) * LANES]
            total[t] = part if i == 0 else total[t] + part
    owners = keep_ref.shape[0]
    for t in range(tiles):
        for j in range(2):
            even = total[t, pl.ds(j, owners, stride=4), :]
            odd = total[t, pl.ds(2 + j, owners, stride=4), :]
            keep_ref[:, 2 * t + j, :] = jnp.where(core == 0, even, odd)
            send_ref[:, 2 * t + j, :] = jnp.where(core == 0, odd, even)


def device_term(small_cols, wide_cols, token_counts):
    tokens, width = small_cols.shape
    d = wide_cols.shape[2]
    steps = tokens // STEP_TOKENS
    half = jax.ShapeDtypeStruct((width // 4, 2 * d // LANES, LANES), jnp.float32)
    return pl.pallas_call(
        term_kernel,
        out_shape=(half, half),
        in_specs=[SMEM, HBM, HBM],
        out_specs=(VMEM, VMEM),
        scratch_shapes=[
            pltpu.VMEM((tokens, width), jnp.bfloat16),
            pltpu.VMEM((tokens, 2, d), jnp.bfloat16),
            pltpu.VMEM((width, 2 * tokens), jnp.bfloat16),
            pltpu.VMEM((d // LANES, width, LANES), jnp.float32),
            pltpu.SemaphoreType.DMA((steps,)),
            pltpu.SemaphoreType.DMA,
        ],
        compiler_params=pltpu.CompilerParams(vmem_limit_bytes=16 * 2**20),
        name="term",
    )(token_counts, in_hbm(small_cols), in_hbm(wide_cols))


def correction(step, log_beta):
    u = step * log_beta
    series = jnp.ones_like(u)
    for k in range(11, 1, -1):
        series = 1.0 + (u / k) * series
    return jnp.where(u > -0.5, -u * series, 1.0 - jnp.exp(u))


def chip_kernel(count_ref, loss_ref, step_ref, keep_ref, got_ref, sum_ref, extra_ref):
    sum_ref[...] = keep_ref[...] + got_ref[...]
    lane = lax.broadcasted_iota(jnp.int32, extra_ref.shape, 1)
    scales = correction(step_ref[...], jnp.where(lane == 3, LOG_FIRST, LOG_SECOND))
    count = count_ref[0].astype(jnp.float32)
    extra_ref[...] = jnp.where(lane == 0, count, jnp.where(lane == 1, loss_ref[0], scales))


def chip_sum(token_counts, loss_sums, step, keep, got):
    return pl.pallas_call(
        chip_kernel,
        out_shape=(
            jax.ShapeDtypeStruct(keep.shape, jnp.float32),
            jax.ShapeDtypeStruct((8, LANES), jnp.float32),
        ),
        in_specs=[SMEM, SMEM, VMEM, VMEM, VMEM],
        out_specs=(VMEM, VMEM),
        compiler_params=pltpu.CompilerParams(vmem_limit_bytes=4 * 2**20),
        name="chip",
    )(token_counts, loss_sums, step, keep, got)


def owned_kernel(extra_ref, parts_ref, out_ref):
    rows = parts_ref.shape[1]
    total = jnp.sum(parts_ref[...], axis=0)
    extra = extra_ref[...]
    for k in range(out_ref.shape[0]):
        out_ref[k, 0:rows, :] = total
        out_ref[k, rows:, :] = extra


def owned(extra, parts, replicas):
    rows = parts.shape[1] + extra.shape[0]
    return pl.pallas_call(
        owned_kernel,
        out_shape=jax.ShapeDtypeStruct((replicas, rows, LANES), jnp.float32),
        in_specs=[VMEM, VMEM],
        out_specs=VMEM,
        compiler_params=pltpu.CompilerParams(vmem_limit_bytes=4 * 2**20),
        name="owned",
    )(extra, parts)


def square_kernel(parts_ref, summed_ref, message_ref):
    rows = summed_ref.shape[0]
    total = jnp.sum(parts_ref[...], axis=0)
    summed = total[:rows]
    summed_ref[...] = summed
    squares = jnp.sum(summed * summed)
    lane = lax.broadcasted_iota(jnp.int32, (1, LANES), 1)
    shifted = total[rows : rows + 1]
    message = jnp.where(lane == 2, squares, shifted)
    message_ref[...] = jnp.broadcast_to(message, message_ref.shape)


def square(parts, owners):
    rows = parts.shape[1] - 8
    return pl.pallas_call(
        square_kernel,
        out_shape=(
            jax.ShapeDtypeStruct((rows, LANES), jnp.float32),
            jax.ShapeDtypeStruct((owners, LANES), jnp.float32),
        ),
        in_specs=[VMEM],
        out_specs=(VMEM, VMEM),
        compiler_params=pltpu.CompilerParams(vmem_limit_bytes=4 * 2**20),
        name="square",
    )(parts)


def update_kernel(
    extra_ref,
    message_ref,
    summed_ref,
    weight_ref,
    first_ref,
    second_ref,
    new_weight_ref,
    new_first_ref,
    new_second_ref,
    adam_ref,
    norm_ref,
    loss_ref,
    rows_ref,
):
    first_scale, second_scale = extra_ref[0:1, 3:4], extra_ref[0:1, 4:5]
    sums = jnp.sum(message_ref[...], axis=0, keepdims=True)
    lane = lax.broadcasted_iota(jnp.int32, sums.shape, 1)

    def take(k):
        return jnp.sum(jnp.where(lane == k, sums, 0.0), axis=1, keepdims=True)

    token_total, loss_total, squares = take(0), take(1), take(2)
    grad_norm = jnp.sqrt(squares) / token_total
    clip = jnp.minimum(1.0, MAX_NORM / (grad_norm + 1e-06))
    norm_ref[...] = grad_norm
    loss_ref[...] = loss_total / token_total
    for t in range(rows_ref.shape[1] // LANES):
        rows_ref[:, t * LANES : (t + 1) * LANES] = summed_ref[2 * t : 2 * t + 2, :]
    clipped = rows_ref[...] / token_total * clip
    new_first = BETA_FIRST * first_ref[...] + (1.0 - BETA_FIRST) * clipped
    new_second = BETA_SECOND * second_ref[...] + (1.0 - BETA_SECOND) * clipped * clipped
    first_hat = new_first / first_scale
    second_hat = new_second / second_scale
    weight = weight_ref[...]
    adam = first_hat / (jnp.sqrt(second_hat) + EPSILON_ADAM) + DECAY_RATE * weight
    new_weight_ref[...] = weight - LEARN_RATE * adam
    new_first_ref[...] = new_first
    new_second_ref[...] = new_second
    adam_ref[...] = adam


def update(extra, message, summed, weight, first_moment, second_moment):
    state = jax.ShapeDtypeStruct(weight.shape, jnp.float32)
    scalar = jax.ShapeDtypeStruct((1, 1), jnp.float32)
    return pl.pallas_call(
        update_kernel,
        out_shape=(state, state, state, state, scalar, scalar),
        in_specs=[VMEM] * 6,
        out_specs=(VMEM,) * 6,
        scratch_shapes=[pltpu.VMEM(weight.shape, jnp.float32)],
        compiler_params=pltpu.CompilerParams(vmem_limit_bytes=4 * 2**20),
        name="update",
    )(extra, message, summed, weight, first_moment, second_moment)


def on_device(
    small_cols, wide_cols, token_counts, loss_sums, weight, first_moment, second_moment, step
):
    owners, replicas = lax.axis_size("fsdp"), lax.axis_size("dp")
    keep, send = device_term(small_cols, wide_cols, token_counts)
    partner = [(i, i ^ 1) for i in range(owners)]
    got = lax.ppermute(send, "fsdp", partner)
    chip, extra = chip_sum(token_counts, loss_sums, jnp.broadcast_to(step.astype(jnp.float32), (8, LANES)), keep, got)
    same_core = [list(range(c, owners, 2)) for c in range(2)]
    parts = lax.all_to_all(chip, "fsdp", 0, 0, axis_index_groups=same_core, tiled=True)
    parts = lax.all_to_all(owned(extra, parts, replicas), "dp", 0, 0, tiled=True)
    summed, message = square(parts, owners)
    message = lax.all_to_all(message[:, None, :], "fsdp", 0, 0, tiled=True)[:, 0, :]
    new_weight, new_first, new_second, adam_step, grad_norm, mean_loss = update(
        extra,
        message,
        summed,
        weight,
        first_moment,
        second_moment,
    )
    return (
        new_weight,
        new_first,
        new_second,
        adam_step,
        grad_norm.reshape(()),
        mean_loss.reshape(()),
    )


def solution(mesh):
    in_specs = (
        P(("dp", "fsdp"), None),
        P(("dp", "fsdp"), None, None),
        P(("dp", "fsdp")),
        P(("dp", "fsdp")),
        P("fsdp", None),
        P("fsdp", None),
        P("fsdp", None),
        P(),
    )
    out_specs = (P("fsdp", None), P("fsdp", None), P("fsdp", None), P("fsdp", None), P(), P())
    return jax.shard_map(
        on_device, mesh=mesh, in_specs=in_specs, out_specs=out_specs, check_vma=False
    )
```

```python
import functools
import math

import jax
import jax.numpy as jnp
from jax import lax
from jax.experimental import pallas as pl
from jax.experimental.pallas import tpu as pltpu
from jax.sharding import PartitionSpec as P

MAX_NORM = 1.0
BETA_FIRST = 0.9
BETA_SECOND = 0.999
EPSILON_ADAM = 1e-08
LEARN_RATE = 0.02
DECAY_RATE = 0.1
LOG_FIRST = -0.10536054214877988
LOG_SECOND = -0.0010004874460928543

LANES = 128
STEP_TOKENS = 384
VMEM = pl.BlockSpec(memory_space=pltpu.VMEM)
HBM = pl.BlockSpec(memory_space=pltpu.HBM)
SMEM = pl.BlockSpec(memory_space=pltpu.SMEM)


def in_hbm(array):
    return pltpu.with_memory_space_constraint(array, pltpu.HBM)


def term_kernel(
    count_ref,
    small_ref,
    wide_ref,
    keep_ref,
    send_ref,
    small_vmem,
    wide_vmem,
    narrow,
    total,
    sems,
    small_sem,
):
    tokens, width = small_ref.shape
    steps = sems.shape[0]
    each = tokens // steps
    core = lax.rem(lax.axis_index("fsdp"), 2)
    small_copy = pltpu.make_async_copy(small_ref, small_vmem, small_sem)
    copies = [
        pltpu.make_async_copy(
            wide_ref.at[pl.ds(i * each, each)], wide_vmem.at[pl.ds(i * each, each)], sems.at[i]
        )
        for i in range(steps)
    ]
    small_copy.start()
    for c in copies:
        c.start()
    live = count_ref[0]
    small_copy.wait()
    block = 128
    for i in range(tokens // block):
        token = lax.broadcasted_iota(jnp.int32, (block, 2 * block), 0)
        slot = lax.broadcasted_iota(jnp.int32, (block, 2 * block), 1)
        twice = jnp.where((slot // 2 == token) & (token + i * block < live), 1.0, 0.0)
        rows = lax.dot_general(
            small_vmem[i * block : (i + 1) * block, :],
            twice.astype(jnp.bfloat16),
            (((0,), (0,)), ((), ())),
            preferred_element_type=jnp.float32,
        )
        row = lax.broadcasted_iota(jnp.int32, (width, 2 * block), 0)
        slot = lax.broadcasted_iota(jnp.int32, (width, 2 * block), 1)
        rows = jnp.where(slot % 2 == row // (width // 2), rows, 0.0)
        narrow[:, 2 * block * i : 2 * block * (i + 1)] = rows.astype(jnp.bfloat16)
    tiles = total.shape[0]
    for i in range(steps):
        copies[i].wait()
        broad = wide_vmem[i * each : (i + 1) * each].reshape(2 * each, tiles * LANES)
        term = jnp.dot(
            narrow[:, 2 * each * i : 2 * each * (i + 1)], broad, preferred_element_type=jnp.float32
        )
        for t in range(tiles):
            part = term[:, t * LANES : (t + 1) * LANES]
            total[t] = part if i == 0 else total[t] + part
    owners = keep_ref.shape[0]
    for t in range(tiles):
        for j in range(2):
            even = total[t, pl.ds(j, owners, stride=4), :]
            odd = total[t, pl.ds(2 + j, owners, stride=4), :]
            keep_ref[:, 2 * t + j, :] = jnp.where(core == 0, even, odd)
            send_ref[:, 2 * t + j, :] = jnp.where(core == 0, odd, even)


def device_term(small_cols, wide_cols, token_counts):
    tokens, width = small_cols.shape
    d = wide_cols.shape[2]
    steps = tokens // STEP_TOKENS
    half = jax.ShapeDtypeStruct((width // 4, 2 * d // LANES, LANES), jnp.float32)
    return pl.pallas_call(
        term_kernel,
        out_shape=(half, half),
        in_specs=[SMEM, HBM, HBM],
        out_specs=(VMEM, VMEM),
        scratch_shapes=[
            pltpu.VMEM((tokens, width), jnp.bfloat16),
            pltpu.VMEM((tokens, 2, d), jnp.bfloat16),
            pltpu.VMEM((width, 2 * tokens), jnp.bfloat16),
            pltpu.VMEM((d // LANES, width, LANES), jnp.float32),
            pltpu.SemaphoreType.DMA((steps,)),
            pltpu.SemaphoreType.DMA,
        ],
        compiler_params=pltpu.CompilerParams(vmem_limit_bytes=16 * 2**20),
        name="term",
    )(token_counts, in_hbm(small_cols), in_hbm(wide_cols))


def correction(step, log_beta):
    u = step * log_beta
    series = jnp.ones_like(u)
    for k in range(11, 1, -1):
        series = 1.0 + (u / k) * series
    return jnp.where(u > -0.5, -u * series, 1.0 - jnp.exp(u))


def chip_kernel(count_ref, loss_ref, step_ref, keep_ref, got_ref, sum_ref, extra_ref):
    sum_ref[...] = keep_ref[...] + got_ref[...]
    lane = lax.broadcasted_iota(jnp.int32, extra_ref.shape, 1)
    scales = correction(step_ref[...], jnp.where(lane == 3, LOG_FIRST, LOG_SECOND))
    count = count_ref[0].astype(jnp.float32)
    extra_ref[...] = jnp.where(lane == 0, count, jnp.where(lane == 1, loss_ref[0], scales))


def chip_sum(token_counts, loss_sums, step, keep, got):
    return pl.pallas_call(
        chip_kernel,
        out_shape=(
            jax.ShapeDtypeStruct(keep.shape, jnp.float32),
            jax.ShapeDtypeStruct((8, LANES), jnp.float32),
        ),
        in_specs=[SMEM, SMEM, VMEM, VMEM, VMEM],
        out_specs=(VMEM, VMEM),
        compiler_params=pltpu.CompilerParams(vmem_limit_bytes=4 * 2**20),
        name="chip",
    )(token_counts, loss_sums, step, keep, got)


def owned_kernel(extra_ref, parts_ref, out_ref):
    rows = parts_ref.shape[1]
    replicas = out_ref.shape[0]
    total = jnp.sum(parts_ref[...], axis=0)
    for r in range(rows):
        row = jnp.broadcast_to(total[r : r + 1][None], (replicas, 1, LANES))
        out_ref[:, :, r * LANES : (r + 1) * LANES] = row
    row = jnp.broadcast_to(extra_ref[0:1][None], (replicas, 1, LANES))
    out_ref[:, :, rows * LANES :] = row


def owned(extra, parts, replicas):
    columns = (parts.shape[1] + 1) * LANES
    return pl.pallas_call(
        owned_kernel,
        out_shape=jax.ShapeDtypeStruct((replicas, 1, columns), jnp.float32),
        in_specs=[VMEM, VMEM],
        out_specs=VMEM,
        compiler_params=pltpu.CompilerParams(vmem_limit_bytes=4 * 2**20),
        name="owned",
    )(extra, parts)


def square_kernel(parts_ref, summed_ref, message_ref):
    rows = summed_ref.shape[0]
    for r in range(rows):
        part = parts_ref[:, :, r * LANES : (r + 1) * LANES]
        summed_ref[r : r + 1, :] = jnp.sum(part, axis=0)
    summed = summed_ref[...]
    squares = jnp.sum(summed * summed)
    lane = lax.broadcasted_iota(jnp.int32, (1, LANES), 1)
    shifted = jnp.sum(parts_ref[:, :, rows * LANES :], axis=0)
    message = jnp.where(lane == 2, squares, shifted)
    message_ref[...] = jnp.broadcast_to(message, message_ref.shape)


def square(parts, owners):
    rows = parts.shape[2] // LANES - 1
    return pl.pallas_call(
        square_kernel,
        out_shape=(
            jax.ShapeDtypeStruct((rows, LANES), jnp.float32),
            jax.ShapeDtypeStruct((owners, LANES), jnp.float32),
        ),
        in_specs=[VMEM],
        out_specs=(VMEM, VMEM),
        compiler_params=pltpu.CompilerParams(vmem_limit_bytes=4 * 2**20),
        name="square",
    )(parts)


def update_kernel(
    extra_ref,
    message_ref,
    summed_ref,
    weight_ref,
    first_ref,
    second_ref,
    new_weight_ref,
    new_first_ref,
    new_second_ref,
    adam_ref,
    norm_ref,
    loss_ref,
    rows_ref,
):
    first_scale, second_scale = extra_ref[0:1, 3:4], extra_ref[0:1, 4:5]
    sums = jnp.sum(message_ref[...], axis=0, keepdims=True)
    lane = lax.broadcasted_iota(jnp.int32, sums.shape, 1)

    def take(k):
        return jnp.sum(jnp.where(lane == k, sums, 0.0), axis=1, keepdims=True)

    token_total, loss_total, squares = take(0), take(1), take(2)
    grad_norm = jnp.sqrt(squares) / token_total
    clip = jnp.minimum(1.0, MAX_NORM / (grad_norm + 1e-06))
    norm_ref[...] = grad_norm
    loss_ref[...] = loss_total / token_total
    for t in range(rows_ref.shape[1] // LANES):
        rows_ref[:, t * LANES : (t + 1) * LANES] = summed_ref[2 * t : 2 * t + 2, :]
    clipped = rows_ref[...] / token_total * clip
    new_first = BETA_FIRST * first_ref[...] + (1.0 - BETA_FIRST) * clipped
    new_second = BETA_SECOND * second_ref[...] + (1.0 - BETA_SECOND) * clipped * clipped
    first_hat = new_first / first_scale
    second_hat = new_second / second_scale
    weight = weight_ref[...]
    adam = first_hat / (jnp.sqrt(second_hat) + EPSILON_ADAM) + DECAY_RATE * weight
    new_weight_ref[...] = weight - LEARN_RATE * adam
    new_first_ref[...] = new_first
    new_second_ref[...] = new_second
    adam_ref[...] = adam


def update(extra, message, summed, weight, first_moment, second_moment):
    state = jax.ShapeDtypeStruct(weight.shape, jnp.float32)
    scalar = jax.ShapeDtypeStruct((1, 1), jnp.float32)
    return pl.pallas_call(
        update_kernel,
        out_shape=(state, state, state, state, scalar, scalar),
        in_specs=[VMEM] * 6,
        out_specs=(VMEM,) * 6,
        scratch_shapes=[pltpu.VMEM(weight.shape, jnp.float32)],
        compiler_params=pltpu.CompilerParams(vmem_limit_bytes=4 * 2**20),
        name="update",
    )(extra, message, summed, weight, first_moment, second_moment)


def on_device(
    small_cols, wide_cols, token_counts, loss_sums, weight, first_moment, second_moment, step
):
    owners, replicas = lax.axis_size("fsdp"), lax.axis_size("dp")
    keep, send = device_term(small_cols, wide_cols, token_counts)
    partner = [(i, i ^ 1) for i in range(owners)]
    got = lax.ppermute(send, "fsdp", partner)
    chip, extra = chip_sum(token_counts, loss_sums, jnp.broadcast_to(step.astype(jnp.float32), (8, LANES)), keep, got)
    same_core = [list(range(c, owners, 2)) for c in range(2)]
    parts = lax.all_to_all(chip, "fsdp", 0, 0, axis_index_groups=same_core, tiled=True)
    parts = lax.all_to_all(owned(extra, parts, replicas), "dp", 0, 0, tiled=True)
    summed, message = square(parts, owners)
    message = lax.all_to_all(message[:, None, :], "fsdp", 0, 0, tiled=True)[:, 0, :]
    new_weight, new_first, new_second, adam_step, grad_norm, mean_loss = update(
        extra,
        message,
        summed,
        weight,
        first_moment,
        second_moment,
    )
    return (
        new_weight,
        new_first,
        new_second,
        adam_step,
        grad_norm.reshape(()),
        mean_loss.reshape(()),
    )


def solution(mesh):
    in_specs = (
        P(("dp", "fsdp"), None),
        P(("dp", "fsdp"), None, None),
        P(("dp", "fsdp")),
        P(("dp", "fsdp")),
        P("fsdp", None),
        P("fsdp", None),
        P("fsdp", None),
        P(),
    )
    out_specs = (P("fsdp", None), P("fsdp", None), P("fsdp", None), P("fsdp", None), P(), P())
    return jax.shard_map(
        on_device, mesh=mesh, in_specs=in_specs, out_specs=out_specs, check_vma=False
    )
```

```python
import functools
import math

import jax
import jax.numpy as jnp
from jax import lax
from jax.experimental import pallas as pl
from jax.experimental.pallas import tpu as pltpu
from jax.sharding import PartitionSpec as P

MAX_NORM = 1.0
BETA_FIRST = 0.9
BETA_SECOND = 0.999
EPSILON_ADAM = 1e-08
LEARN_RATE = 0.02
DECAY_RATE = 0.1
LOG_FIRST = -0.10536054214877988
LOG_SECOND = -0.0010004874460928543

LANES = 128
STEP_TOKENS = 384
VMEM = pl.BlockSpec(memory_space=pltpu.VMEM)
HBM = pl.BlockSpec(memory_space=pltpu.HBM)
SMEM = pl.BlockSpec(memory_space=pltpu.SMEM)


def in_hbm(array):
    return pltpu.with_memory_space_constraint(array, pltpu.HBM)


def term_kernel(
    count_ref,
    small_ref,
    wide_ref,
    total_ref,
    send_ref,
    small_vmem,
    wide_vmem,
    narrow,
    sems,
    small_sem,
):
    tokens, width = small_ref.shape
    steps = sems.shape[0]
    each = tokens // steps
    core = lax.rem(lax.axis_index("fsdp"), 2)
    small_copy = pltpu.make_async_copy(small_ref, small_vmem, small_sem)
    copies = [
        pltpu.make_async_copy(
            wide_ref.at[pl.ds(i * each, each)], wide_vmem.at[pl.ds(i * each, each)], sems.at[i]
        )
        for i in range(steps)
    ]
    small_copy.start()
    for c in copies:
        c.start()
    live = count_ref[0]
    small_copy.wait()
    block = 128
    for i in range(tokens // block):
        token = lax.broadcasted_iota(jnp.int32, (block, 2 * block), 0)
        slot = lax.broadcasted_iota(jnp.int32, (block, 2 * block), 1)
        twice = jnp.where((slot // 2 == token) & (token + i * block < live), 1.0, 0.0)
        rows = lax.dot_general(
            small_vmem[i * block : (i + 1) * block, :],
            twice.astype(jnp.bfloat16),
            (((0,), (0,)), ((), ())),
            preferred_element_type=jnp.float32,
        )
        row = lax.broadcasted_iota(jnp.int32, (width, 2 * block), 0)
        slot = lax.broadcasted_iota(jnp.int32, (width, 2 * block), 1)
        rows = jnp.where(slot % 2 == row // (width // 2), rows, 0.0)
        narrow[:, 2 * block * i : 2 * block * (i + 1)] = rows.astype(jnp.bfloat16)
    tiles = total_ref.shape[1]
    for i in range(steps):
        copies[i].wait()
        broad = wide_vmem[i * each : (i + 1) * each].reshape(2 * each, tiles * LANES)
        term = jnp.dot(
            narrow[:, 2 * each * i : 2 * each * (i + 1)], broad, preferred_element_type=jnp.float32
        )
        for t in range(tiles):
            total_ref[i, t] = term[:, t * LANES : (t + 1) * LANES]
    take_half(total_ref, 1 - core, send_ref)


def take_half(total_ref, column, half_ref):
    owners = half_ref.shape[0]
    for t in range(total_ref.shape[1]):
        for j in range(2):
            rows = pl.ds(2 * column + j, owners, stride=4)
            half_ref[:, 2 * t + j, :] = sum(
                total_ref[i, t, rows, :] for i in range(total_ref.shape[0])
            )


def keep_kernel(total_ref, keep_ref):
    take_half(total_ref, lax.rem(lax.axis_index("fsdp"), 2), keep_ref)


def kept(total, half):
    return pl.pallas_call(
        keep_kernel,
        out_shape=jax.ShapeDtypeStruct(half.shape, half.dtype),
        in_specs=[VMEM],
        out_specs=VMEM,
        cost_estimate=pl.CostEstimate(flops=10**8, bytes_accessed=10**6, transcendentals=0),
        compiler_params=pltpu.CompilerParams(vmem_limit_bytes=4 * 2**20),
        name="keep",
    )(total)


def device_term(small_cols, wide_cols, token_counts):
    tokens, width = small_cols.shape
    d = wide_cols.shape[2]
    steps = tokens // STEP_TOKENS
    half = jax.ShapeDtypeStruct((width // 4, 2 * d // LANES, LANES), jnp.float32)
    return pl.pallas_call(
        term_kernel,
        out_shape=(
            jax.ShapeDtypeStruct((steps, d // LANES, width, LANES), jnp.float32),
            half,
        ),
        in_specs=[SMEM, HBM, HBM],
        out_specs=(VMEM, VMEM),
        scratch_shapes=[
            pltpu.VMEM((tokens, width), jnp.bfloat16),
            pltpu.VMEM((tokens, 2, d), jnp.bfloat16),
            pltpu.VMEM((width, 2 * tokens), jnp.bfloat16),
            pltpu.SemaphoreType.DMA((steps,)),
            pltpu.SemaphoreType.DMA,
        ],
        compiler_params=pltpu.CompilerParams(vmem_limit_bytes=16 * 2**20),
        name="term",
    )(token_counts, in_hbm(small_cols), in_hbm(wide_cols))


def correction(step, log_beta):
    u = step * log_beta
    series = jnp.ones_like(u)
    for k in range(11, 1, -1):
        series = 1.0 + (u / k) * series
    return jnp.where(u > -0.5, -u * series, 1.0 - jnp.exp(u))


def chip_kernel(count_ref, loss_ref, step_ref, keep_ref, got_ref, sum_ref, extra_ref):
    sum_ref[...] = keep_ref[...] + got_ref[...]
    lane = lax.broadcasted_iota(jnp.int32, extra_ref.shape, 1)
    scales = correction(step_ref[...], jnp.where(lane == 3, LOG_FIRST, LOG_SECOND))
    count = count_ref[0].astype(jnp.float32)
    extra_ref[...] = jnp.where(lane == 0, count, jnp.where(lane == 1, loss_ref[0], scales))


def chip_sum(token_counts, loss_sums, step, keep, got):
    return pl.pallas_call(
        chip_kernel,
        out_shape=(
            jax.ShapeDtypeStruct(keep.shape, jnp.float32),
            jax.ShapeDtypeStruct((8, LANES), jnp.float32),
        ),
        in_specs=[SMEM, SMEM, VMEM, VMEM, VMEM],
        out_specs=(VMEM, VMEM),
        compiler_params=pltpu.CompilerParams(vmem_limit_bytes=4 * 2**20),
        name="chip",
    )(token_counts, loss_sums, step, keep, got)


def owned_kernel(extra_ref, parts_ref, out_ref):
    rows = parts_ref.shape[1]
    replicas = out_ref.shape[0]
    total = jnp.sum(parts_ref[...], axis=0)
    for r in range(rows):
        row = jnp.broadcast_to(total[r : r + 1][None], (replicas, 1, LANES))
        out_ref[:, :, r * LANES : (r + 1) * LANES] = row
    row = jnp.broadcast_to(extra_ref[0:1][None], (replicas, 1, LANES))
    out_ref[:, :, rows * LANES :] = row


def owned(extra, parts, replicas):
    columns = (parts.shape[1] + 1) * LANES
    return pl.pallas_call(
        owned_kernel,
        out_shape=jax.ShapeDtypeStruct((replicas, 1, columns), jnp.float32),
        in_specs=[VMEM, VMEM],
        out_specs=VMEM,
        compiler_params=pltpu.CompilerParams(vmem_limit_bytes=4 * 2**20),
        name="owned",
    )(extra, parts)


def square_kernel(parts_ref, summed_ref, message_ref):
    rows = summed_ref.shape[0]
    for r in range(rows):
        part = parts_ref[:, :, r * LANES : (r + 1) * LANES]
        summed_ref[r : r + 1, :] = jnp.sum(part, axis=0)
    summed = summed_ref[...]
    squares = jnp.sum(summed * summed)
    lane = lax.broadcasted_iota(jnp.int32, (1, LANES), 1)
    shifted = jnp.sum(parts_ref[:, :, rows * LANES :], axis=0)
    message = jnp.where(lane == 2, squares, shifted)
    message_ref[...] = jnp.broadcast_to(message, message_ref.shape)


def square(parts, owners):
    rows = parts.shape[2] // LANES - 1
    return pl.pallas_call(
        square_kernel,
        out_shape=(
            jax.ShapeDtypeStruct((rows, LANES), jnp.float32),
            jax.ShapeDtypeStruct((owners, LANES), jnp.float32),
        ),
        in_specs=[VMEM],
        out_specs=(VMEM, VMEM),
        compiler_params=pltpu.CompilerParams(vmem_limit_bytes=4 * 2**20),
        name="square",
    )(parts)


def update_kernel(
    extra_ref,
    message_ref,
    summed_ref,
    weight_ref,
    first_ref,
    second_ref,
    new_weight_ref,
    new_first_ref,
    new_second_ref,
    adam_ref,
    norm_ref,
    loss_ref,
    rows_ref,
):
    first_scale, second_scale = extra_ref[0:1, 3:4], extra_ref[0:1, 4:5]
    sums = jnp.sum(message_ref[...], axis=0, keepdims=True)
    lane = lax.broadcasted_iota(jnp.int32, sums.shape, 1)

    def take(k):
        return jnp.sum(jnp.where(lane == k, sums, 0.0), axis=1, keepdims=True)

    token_total, loss_total, squares = take(0), take(1), take(2)
    grad_norm = jnp.sqrt(squares) / token_total
    clip = jnp.minimum(1.0, MAX_NORM / (grad_norm + 1e-06))
    norm_ref[...] = grad_norm
    loss_ref[...] = loss_total / token_total
    for t in range(rows_ref.shape[1] // LANES):
        rows_ref[:, t * LANES : (t + 1) * LANES] = summed_ref[2 * t : 2 * t + 2, :]
    clipped = rows_ref[...] / token_total * clip
    new_first = BETA_FIRST * first_ref[...] + (1.0 - BETA_FIRST) * clipped
    new_second = BETA_SECOND * second_ref[...] + (1.0 - BETA_SECOND) * clipped * clipped
    first_hat = new_first / first_scale
    second_hat = new_second / second_scale
    weight = weight_ref[...]
    adam = first_hat / (jnp.sqrt(second_hat) + EPSILON_ADAM) + DECAY_RATE * weight
    new_weight_ref[...] = weight - LEARN_RATE * adam
    new_first_ref[...] = new_first
    new_second_ref[...] = new_second
    adam_ref[...] = adam


def update(extra, message, summed, weight, first_moment, second_moment):
    state = jax.ShapeDtypeStruct(weight.shape, jnp.float32)
    scalar = jax.ShapeDtypeStruct((1, 1), jnp.float32)
    return pl.pallas_call(
        update_kernel,
        out_shape=(state, state, state, state, scalar, scalar),
        in_specs=[VMEM] * 6,
        out_specs=(VMEM,) * 6,
        scratch_shapes=[pltpu.VMEM(weight.shape, jnp.float32)],
        compiler_params=pltpu.CompilerParams(vmem_limit_bytes=4 * 2**20),
        name="update",
    )(extra, message, summed, weight, first_moment, second_moment)


def on_device(
    small_cols, wide_cols, token_counts, loss_sums, weight, first_moment, second_moment, step
):
    owners, replicas = lax.axis_size("fsdp"), lax.axis_size("dp")
    total, send = device_term(small_cols, wide_cols, token_counts)
    partner = [(i, i ^ 1) for i in range(owners)]
    got = lax.ppermute(send, "fsdp", partner)
    keep = kept(total, send)
    chip, extra = chip_sum(token_counts, loss_sums, jnp.broadcast_to(step.astype(jnp.float32), (8, LANES)), keep, got)
    same_core = [list(range(c, owners, 2)) for c in range(2)]
    parts = lax.all_to_all(chip, "fsdp", 0, 0, axis_index_groups=same_core, tiled=True)
    parts = lax.all_to_all(owned(extra, parts, replicas), "dp", 0, 0, tiled=True)
    summed, message = square(parts, owners)
    message = lax.all_to_all(message[:, None, :], "fsdp", 0, 0, tiled=True)[:, 0, :]
    new_weight, new_first, new_second, adam_step, grad_norm, mean_loss = update(
        extra,
        message,
        summed,
        weight,
        first_moment,
        second_moment,
    )
    return (
        new_weight,
        new_first,
        new_second,
        adam_step,
        grad_norm.reshape(()),
        mean_loss.reshape(()),
    )


def solution(mesh):
    in_specs = (
        P(("dp", "fsdp"), None),
        P(("dp", "fsdp"), None, None),
        P(("dp", "fsdp")),
        P(("dp", "fsdp")),
        P("fsdp", None),
        P("fsdp", None),
        P("fsdp", None),
        P(),
    )
    out_specs = (P("fsdp", None), P("fsdp", None), P("fsdp", None), P("fsdp", None), P(), P())
    return jax.shard_map(
        on_device, mesh=mesh, in_specs=in_specs, out_specs=out_specs, check_vma=False
    )
```
